128 devices in a mesh: row: 16 (over y, z), col: 8 (over x, core).
Axes of the slice: x: 4, y: 4, z: 4, core: 2. Of those that a mesh axis runs over, the one named last changes fastest.
Arguments:
- matrix_tiles: bfloat16 [16, 8, 96, 256, 256], P('row', 'col'), may hold values from -0.0546875 to 0.0546875
- tile_rows: int32 [16, 8, 96], P('row', 'col'), may hold values from 0 to 7, as said below
- tile_cols: int32 [16, 8, 96], P('row', 'col'), may hold values from 0 to 15
- tile_count: int32 [16, 8], P('row', 'col'), may hold values from 24 to 96, as said below
- x_start: float32 [32768, 256], P(('col', 'row')), may hold values from -5 to 5
- y_start: float32 [32768, 256], P(('row', 'col')), may hold values from 0 to 1
- cost_vector: float32 [32768, 256], P(('col', 'row')), may hold values from -6 to 6
- right_side: float32 [32768, 256], P(('row', 'col')), may hold values from -6 to 6
- lower_bound: float32 [32768, 256], P(('col', 'row')), may hold values from -1.5 to -0.3
- upper_bound: float32 [32768, 256], P(('col', 'row')), may hold values from 0.3 to 1.5
- step_primal: float32 [256], replicated, may hold values from 0.2 to 0.45
- step_dual: float32 [256], replicated, may hold values from 0.2 to 0.45
Outputs:
- primal_out: float32 [32768, 256], P(('col', 'row'))
- dual_out: float32 [32768, 256], P(('row', 'col'))
The draws below stay inside these ranges and needn't reach their ends.
Inputs may be any that keep to these rules, and one draw needn't show every extreme that they name: Within one grid cell the pairs (tile_rows, tile_cols) of its slots are all different. `tile_count`: some grid cell has 96 used slots in every draw; slots at or above a cell's count are not part of A.
All inputs are finite; a program needn't handle non-finite values.
Results may differ from the reference program's by a relative error of at most 0.001.
Values may be sent and summed in bfloat16 or wider, within the bound.
No kernel may reach another device: no remote copies, remote signals or barrier semaphores. Data moves between devices by JAX's collectives and lax.ppermute only.
A program may use at most 128 MiB of HBM per device.

```python
import math
import jax
import jax.numpy as jnp
from jax import lax

TILE = 256
NR_DEV = 8
NC_DEV = 16
TILES_MAX = 96
BATCH = 256
ROWS = 32768
COLS = 32768
N_ROW = 16
N_COL = 8


def tile_places(key):
    key_list = jax.random.split(jax.random.fold_in(key, 7), N_ROW * N_COL)

    def one_cell(cell_key):
        return jax.random.permutation(cell_key, NR_DEV * NC_DEV)[:TILES_MAX]
    shuffled = jax.vmap(one_cell)(key_list)
    return shuffled.reshape(N_ROW, N_COL, TILES_MAX).astype(jnp.int32)


def draw_tile_rows(key, part):
    return (tile_places(key) // NC_DEV).astype(jnp.int32)


def draw_tile_cols(key, part):
    return (tile_places(key) % NC_DEV).astype(jnp.int32)


def draw_tile_count(key, part):
    base_count = jax.random.randint(jax.random.fold_in(key, 3), (N_ROW, N_COL), TILES_MAX // 4, TILES_MAX // 2 + 1)
    heavy_cell = jax.random.randint(jax.random.fold_in(key, 5), (N_ROW, N_COL), 0, 8) == 0
    chosen = jax.random.randint(jax.random.fold_in(key, 9), (), 0, N_ROW * N_COL)
    picked = jnp.arange(N_ROW * N_COL, dtype=jnp.int32).reshape(N_ROW, N_COL) == chosen
    full_count = jnp.full((N_ROW, N_COL), TILES_MAX, jnp.int32)
    return jnp.where(heavy_cell | picked, full_count, base_count).astype(jnp.int32)


def steps_of(own_key, extent, cuts, least, largest):
    def one(position, blocks):
        heights = jax.random.uniform(jax.random.fold_in(jax.random.fold_in(own_key, 6), position), (blocks,), jnp.float32, least / len(cuts), largest / len(cuts))
        return jnp.repeat(jnp.exp(heights), extent[position] // blocks).reshape((-1,) + (1,) * (len(extent) - position - 1))

    factor_of = one(*cuts[0])
    for cut in cuts[1:]:
        factor_of = factor_of * one(*cut)
    return factor_of


def noise(stream_key, dims, width, reach, cuts=(), kind=jnp.bfloat16):
    level = steps_of(stream_key, dims, cuts, -0.22, 0.18) if cuts else 1.0
    entries = jax.random.normal(stream_key, dims, jnp.float32) * width * level
    return jnp.minimum(jnp.maximum(entries, -reach), reach).astype(kind)


def setup_inputs(seed: int = 0) -> dict:
    streams_of = jax.random.split(jax.random.key(seed), 13)
    return {
        "matrix_tiles": noise(streams_of[0], (N_ROW, N_COL, TILES_MAX, TILE, TILE), (TILE * TILES_MAX * N_COL // (2 * NR_DEV)) ** -0.5, 0.0546875, ((0, 16), (1, 8))),
        "tile_rows": draw_tile_rows(jax.random.fold_in(streams_of[12], 71), 0),
        "tile_cols": draw_tile_cols(jax.random.fold_in(streams_of[12], 71), 0),
        "tile_count": draw_tile_count(jax.random.fold_in(streams_of[12], 71), 0),
        "x_start": noise(streams_of[4], (COLS, BATCH), 0.8, 5.0, ((0, 128),), jnp.float32),
        "y_start": jnp.clip(1.0 * jax.random.uniform(streams_of[5], (ROWS, BATCH), jnp.float32) ** steps_of(streams_of[5], (ROWS, BATCH), ((0, 128),), -0.2, 0.2), 0.0, 1.0),
        "cost_vector": noise(streams_of[6], (COLS, BATCH), 1.0, 6.0, ((0, 128),), jnp.float32),
        "right_side": noise(streams_of[7], (ROWS, BATCH), 1.0, 6.0, ((0, 128),), jnp.float32),
        "lower_bound": jnp.clip(-1.5 + 1.2 * jax.random.uniform(streams_of[8], (COLS, BATCH), jnp.float32) ** steps_of(streams_of[8], (COLS, BATCH), ((0, 128),), -0.2, 0.2), -1.5, -0.3),
        "upper_bound": jnp.clip(0.3 + 1.2 * jax.random.uniform(streams_of[9], (COLS, BATCH), jnp.float32) ** steps_of(streams_of[9], (COLS, BATCH), ((0, 128),), -0.2, 0.2), 0.3, 1.5),
        "step_primal": jnp.clip(jnp.exp(jax.random.uniform(streams_of[10], (BATCH,), jnp.float32, math.log(0.2), math.log(0.45))), 0.2, 0.45),
        "step_dual": jnp.clip(jnp.exp(jax.random.uniform(streams_of[11], (BATCH,), jnp.float32, math.log(0.2), math.log(0.45))), 0.2, 0.45),
    }


def forward_all(matrix_tiles, tile_rows, tile_cols, tile_count, vector):
    x_tiles = vector.astype(jnp.float32).reshape(N_COL * NC_DEV, TILE, -1)
    slot_ids = jnp.arange(TILES_MAX, dtype=jnp.int32)

    def cell(running, flat):
        grid_row = flat // N_COL
        grid_col = flat % N_COL
        block = matrix_tiles[grid_row, grid_col].astype(jnp.float32)
        pieces = x_tiles[grid_col * NC_DEV + tile_cols[grid_row, grid_col]]
        products = jnp.einsum('sij,sjb->sib', block, pieces, precision=lax.Precision.HIGHEST)
        in_use = slot_ids < tile_count[grid_row, grid_col]
        products = jnp.where(in_use[:, None, None], products, jnp.zeros_like(products))
        running = running.at[grid_row * NR_DEV + tile_rows[grid_row, grid_col]].add(products)
        return (running, None)
    begin = jnp.zeros((N_ROW * NR_DEV, TILE, x_tiles.shape[-1]), jnp.float32)
    total, unused = lax.scan(cell, begin, jnp.arange(N_ROW * N_COL, dtype=jnp.int32))
    return total.reshape(ROWS, -1)

def backward_all(matrix_tiles, tile_rows, tile_cols, tile_count, vector):
    y_tiles = vector.astype(jnp.float32).reshape(N_ROW * NR_DEV, TILE, -1)
    slot_ids = jnp.arange(TILES_MAX, dtype=jnp.int32)

    def cell(running, flat):
        grid_row = flat // N_COL
        grid_col = flat % N_COL
        block = matrix_tiles[grid_row, grid_col].astype(jnp.float32)
        pieces = y_tiles[grid_row * NR_DEV + tile_rows[grid_row, grid_col]]
        products = jnp.einsum('sij,sib->sjb', block, pieces, precision=lax.Precision.HIGHEST)
        in_use = slot_ids < tile_count[grid_row, grid_col]
        products = jnp.where(in_use[:, None, None], products, jnp.zeros_like(products))
        running = running.at[grid_col * NC_DEV + tile_cols[grid_row, grid_col]].add(products)
        return (running, None)
    begin = jnp.zeros((N_COL * NC_DEV, TILE, y_tiles.shape[-1]), jnp.float32)
    total, unused = lax.scan(cell, begin, jnp.arange(N_ROW * N_COL, dtype=jnp.int32))
    return total.reshape(COLS, -1)

def reference(matrix_tiles, tile_rows, tile_cols, tile_count, x_start, y_start, cost_vector, right_side, lower_bound, upper_bound, step_primal, step_dual):
    grad_zero = backward_all(matrix_tiles, tile_rows, tile_cols, tile_count, y_start.astype(jnp.bfloat16))
    primal_one = jnp.clip(x_start - step_primal * (cost_vector - grad_zero), lower_bound, upper_bound)
    ahead_one = (2.0 * primal_one - x_start).astype(jnp.bfloat16)
    image_one = forward_all(matrix_tiles, tile_rows, tile_cols, tile_count, ahead_one)
    dual_one = jnp.maximum(y_start + step_dual * (right_side - image_one), 0.0)
    primal_diff = primal_one - x_start
    dual_diff = dual_one - y_start
    move_primal = lax.optimization_barrier(jnp.sum(primal_diff * primal_diff, axis=0))
    move_dual = lax.optimization_barrier(jnp.sum(dual_diff * dual_diff, axis=0))
    weight = jnp.sqrt((move_dual / ROWS + 1e-06) / (move_primal / COLS + 1e-06))
    grad_one = backward_all(matrix_tiles, tile_rows, tile_cols, tile_count, dual_one.astype(jnp.bfloat16))
    primal_out = jnp.clip(primal_one - step_primal / weight * (cost_vector - grad_one), lower_bound, upper_bound)
    ahead_two = (2.0 * primal_out - primal_one).astype(jnp.bfloat16)
    image_two = forward_all(matrix_tiles, tile_rows, tile_cols, tile_count, ahead_two)
    dual_out = jnp.maximum(dual_one + step_dual * weight * (right_side - image_two), 0.0)
    return (primal_out, dual_out)
```

```python
import jax
import jax.numpy as jnp
from jax import lax
from jax.experimental import pallas as pl
from jax.experimental.pallas import tpu as pltpu
from jax.sharding import Mesh
from jax.sharding import PartitionSpec as P

ROW = ("row_0", "row_1")
COL = ("col_0", "col_1")
ROW_COL = ("row_0", "row_1", "col_0", "col_1")
COL_ROW = ("col_0", "col_1", "row_0", "row_1")

NR = 8
NC = 16
T = 256
EXTRA = 16
TALL = T + EXTRA
EPS = 1e-06
f32 = jnp.float32
bf16 = jnp.bfloat16

VMEM = pl.BlockSpec(memory_space=pltpu.VMEM)
SMEM = pl.BlockSpec(memory_space=pltpu.SMEM)
ANY = pl.BlockSpec(memory_space=pl.ANY)


def three_parts(v):
    high = v.astype(bf16)
    rest = v - high.astype(f32)
    middle = rest.astype(bf16)
    low = (rest - middle.astype(f32)).astype(bf16)
    row = lax.broadcasted_iota(jnp.int32, (EXTRA, T), 0)
    out = jnp.where(row == 0, high.astype(f32), 0.0)
    out = jnp.where(row == 1, middle.astype(f32), out)
    return jnp.where(row == 2, low.astype(f32), out).astype(bf16)


def sum_of_parts(ref, count):
    total = ref[0, T:TALL, :].astype(f32)
    for k in range(1, count):
        total = total + ref[k, T:TALL, :].astype(f32)
    return jnp.sum(total, axis=0, keepdims=True)


def copy_of(table, tiles, dense, sems, place):
    r, c = place // NC, place % NC
    return pltpu.make_async_copy(
        tiles.at[table[place]],
        dense.at[r, :, pl.ds(pl.multiple_of(c * T, T), T)],
        sems.at[place],
    )


def start_copy(table, tiles, dense, sems, place):
    @pl.when(table[place] >= 0)
    def _():
        copy_of(table, tiles, dense, sems, place).start()

    @pl.when(table[place] < 0)
    def _():
        r, c = place // NC, place % NC
        dense[r, :, pl.ds(pl.multiple_of(c * T, T), T)] = jnp.zeros((T, T), bf16)


def wait_copy(table, tiles, dense, sems, place):
    @pl.when(table[place] >= 0)
    def _():
        copy_of(table, tiles, dense, sems, place).wait()


ROWS_PER_STEP = 2
COLS_PER_STEP = 2


def forward_kernel(extra, table, tiles, x, out, dense, sems):
    def start(place, carry):
        start_copy(table, tiles, dense, sems, place)
        return carry

    lax.fori_loop(0, NR * NC, start, 0)
    if extra:
        out[:, T:TALL, :] = jnp.broadcast_to(three_parts(sum_of_parts(x, NC))[None], (NR, EXTRA, T))

    def step(i, carry):
        def wait(k, carry):
            wait_copy(table, tiles, dense, sems, i * ROWS_PER_STEP * NC + k)
            return carry

        lax.fori_loop(0, ROWS_PER_STEP * NC, wait, 0)
        left = dense[pl.ds(i * ROWS_PER_STEP, ROWS_PER_STEP)].reshape(ROWS_PER_STEP * T, NC * T)
        right = x[:, :T, :].reshape(NC * T, T)
        product = jnp.dot(left, right, preferred_element_type=f32)
        out[pl.ds(i * ROWS_PER_STEP, ROWS_PER_STEP), :T, :] = product.astype(bf16).reshape(ROWS_PER_STEP, T, T)
        return carry

    lax.fori_loop(0, NR // ROWS_PER_STEP, step, 0)


def backward_kernel(extra, table, tiles, y, out, dense, sems):
    def start(k, carry):
        start_copy(table, tiles, dense, sems, (k % NR) * NC + k // NR)
        return carry

    lax.fori_loop(0, NR * NC, start, 0)
    if extra:
        out[:, T:TALL, :] = jnp.broadcast_to(three_parts(sum_of_parts(y, NR))[None], (NC, EXTRA, T))

    def step(i, carry):
        def wait(k, carry):
            wait_copy(table, tiles, dense, sems, (k % NR) * NC + i * COLS_PER_STEP + k // NR)
            return carry

        lax.fori_loop(0, COLS_PER_STEP * NR, wait, 0)
        left = jnp.concatenate([y[r, :T, :] for r in range(NR)], axis=1)
        width = COLS_PER_STEP * T
        right = dense[:, :, pl.ds(pl.multiple_of(i * width, width), width)].reshape(NR * T, width)
        product = jnp.dot(left, right, preferred_element_type=f32).astype(bf16)
        for k in range(COLS_PER_STEP):
            out[i * COLS_PER_STEP + k, :T, :] = product[:, k * T : (k + 1) * T]
        return carry

    lax.fori_loop(0, NC // COLS_PER_STEP, step, 0)


def multiply(kernel, table, tiles, pieces, outs, extra):
    tall = TALL if extra else T
    return pl.pallas_call(
        lambda *refs: kernel(extra, *refs),
        out_shape=jax.ShapeDtypeStruct((outs, tall, T), bf16),
        in_specs=[SMEM, ANY, VMEM],
        out_specs=VMEM,
        scratch_shapes=[pltpu.VMEM((NR, T, NC * T), bf16), pltpu.SemaphoreType.DMA((NR * NC,))],
        cost_estimate=pl.CostEstimate(flops=2 * NR * NC * T**3, bytes_accessed=NR * NC * T * T * 2, transcendentals=0),
        name=kernel.__name__,
    )(table, tiles, pieces)


def block_sum(ref, count):
    total = ref[0, :T, :].astype(f32)
    for k in range(1, count):
        total = total + ref[k, :T, :].astype(f32)
    return total


def spread(out, block, row=None):
    for k in range(out.shape[0]):
        out[k, :T, :] = block
        if row is not None:
            out[k, T:TALL, :] = row


def primal_one_kernel(pieces, x, cost, low, high, step, primal, ahead):
    grad = block_sum(pieces, NC).T
    one = jnp.clip(x[...] - step[...] * (cost[...] - grad), low[...], high[...])
    primal[...] = one
    diff = one - x[...]
    spread(ahead, (2.0 * one - x[...]).astype(bf16), three_parts(jnp.sum(diff * diff, axis=0, keepdims=True)))


def dual_one_kernel(pieces, y, side, step, dual, moved, flipped):
    image = block_sum(pieces, NR)
    moved[...] = sum_of_parts(pieces, NR)
    one = jnp.maximum(y[...] + step[...] * (side[...] - image), 0.0)
    dual[...] = one
    diff = one - y[...]
    spread(flipped, one.T.astype(bf16), three_parts(jnp.sum(diff * diff, axis=0, keepdims=True)))


def primal_two_kernel(rows, cols, pieces, moved, one, cost, low, high, step, primal, weight, ahead):
    grad = block_sum(pieces, NC).T
    move_dual = sum_of_parts(pieces, NC)
    w = jnp.sqrt((move_dual / rows + EPS) / (moved[...] / cols + EPS))
    weight[...] = w
    two = jnp.clip(one[...] - step[...] / w * (cost[...] - grad), low[...], high[...])
    primal[...] = two
    spread(ahead, (2.0 * two - one[...]).astype(bf16))


def dual_two_kernel(pieces, one, side, step, weight, dual):
    image = block_sum(pieces, NR)
    dual[...] = jnp.maximum(one[...] + step[...] * weight[...] * (side[...] - image), 0.0)


def flip_kernel(y, flipped):
    spread(flipped, y[...].T.astype(bf16))


def call(kernel, outs, *args, name):
    return pl.pallas_call(
        kernel,
        out_shape=[jax.ShapeDtypeStruct(shape, kind) for shape, kind in outs],
        in_specs=[VMEM] * len(args),
        out_specs=[VMEM] * len(outs),
        name=name,
    )(*args)


def exchange(pieces, axis):
    return lax.all_to_all(pieces, axis, 0, 0, tiled=True)


def body(
    matrix_tiles,
    tile_rows,
    tile_cols,
    tile_count,
    x_start,
    y_start,
    cost_vector,
    right_side,
    lower_bound,
    upper_bound,
    step_primal,
    step_dual,
):
    tiles = matrix_tiles[0, 0]
    slots = tiles.shape[0]
    slot = jnp.arange(slots, dtype=jnp.int32)
    place = jnp.where(slot < tile_count[0, 0], tile_rows[0, 0] * NC + tile_cols[0, 0], -1)
    places = jnp.arange(NR * NC, dtype=jnp.int32)
    table = jnp.max(jnp.where(place[None, :] == places[:, None], slot[None, :], -1), axis=1)
    everyone = lax.axis_size(ROW) * lax.axis_size(COL)
    total_cols = x_start.shape[0] * everyone
    total_rows = y_start.shape[0] * everyone
    step_p, step_d = step_primal[None], step_dual[None]
    square = ((T, T), f32)
    line = ((1, T), f32)

    (flipped,) = call(flip_kernel, [((NR, T, T), bf16)], y_start, name="flip")
    flipped = exchange(flipped, COL)
    grads = exchange(multiply(backward_kernel, table, tiles, flipped, NC, False), ROW)
    one, ahead = call(
        primal_one_kernel,
        [square, ((NC, TALL, T), bf16)],
        grads, x_start, cost_vector, lower_bound, upper_bound, step_p,
        name="primal_one",
    )
    ahead = exchange(ahead, ROW)
    images = exchange(multiply(forward_kernel, table, tiles, ahead, NR, True), COL)
    dual, moved, flipped = call(
        dual_one_kernel,
        [square, line, ((NR, TALL, T), bf16)],
        images, y_start, right_side, step_d,
        name="dual_one",
    )
    flipped = exchange(flipped, COL)
    grads = exchange(multiply(backward_kernel, table, tiles, flipped, NC, True), ROW)
    two, weight, ahead = call(
        lambda *refs: primal_two_kernel(float(total_rows), float(total_cols), *refs),
        [square, line, ((NC, T, T), bf16)],
        grads, moved, one, cost_vector, lower_bound, upper_bound, step_p,
        name="primal_two",
    )
    ahead = exchange(ahead, ROW)
    images = exchange(multiply(forward_kernel, table, tiles, ahead, NR, False), COL)
    (dual_out,) = call(dual_two_kernel, [square], images, dual, right_side, step_d, weight, name="dual_two")
    return (two, dual_out)


def solution(mesh):
    torus = Mesh(mesh.devices.reshape(4, 4, 4, 2), ("row_0", "row_1", "col_0", "col_1"))
    in_specs = (
        P(ROW, COL, None, None, None),
        P(ROW, COL, None),
        P(ROW, COL, None),
        P(ROW, COL),
        P(COL_ROW, None),
        P(ROW_COL, None),
        P(COL_ROW, None),
        P(ROW_COL, None),
        P(COL_ROW, None),
        P(COL_ROW, None),
        P(),
        P(),
    )
    out_specs = (P(COL_ROW, None), P(ROW_COL, None))
    return jax.shard_map(body, mesh=torus, in_specs=in_specs, out_specs=out_specs, check_vma=False)
```

```python
import jax
import jax.numpy as jnp
from jax import lax
from jax.experimental import pallas as pl
from jax.experimental.pallas import tpu as pltpu
from jax.sharding import Mesh
from jax.sharding import PartitionSpec as P

ROW = ("row_0", "row_1")
COL = ("col_0", "col_1")
ROW_COL = ("row_0", "row_1", "col_0", "col_1")
COL_ROW = ("col_0", "col_1", "row_0", "row_1")

NR = 8
NC = 16
T = 256
EXTRA = 16
TALL = T + EXTRA
EPS = 1e-06
f32 = jnp.float32
bf16 = jnp.bfloat16

VMEM = pl.BlockSpec(memory_space=pltpu.VMEM)
SMEM = pl.BlockSpec(memory_space=pltpu.SMEM)
MIB = 1 << 20


def three_parts(v):
    high = v.astype(bf16)
    rest = v - high.astype(f32)
    middle = rest.astype(bf16)
    low = (rest - middle.astype(f32)).astype(bf16)
    row = lax.broadcasted_iota(jnp.int32, (EXTRA, T), 0)
    out = jnp.where(row == 0, high.astype(f32), 0.0)
    out = jnp.where(row == 1, middle.astype(f32), out)
    return jnp.where(row == 2, low.astype(f32), out).astype(bf16)


def sum_of_parts(ref, count):
    total = ref[0, T:TALL, :].astype(f32)
    for k in range(1, count):
        total = total + ref[k, T:TALL, :].astype(f32)
    return jnp.sum(total, axis=0, keepdims=True)


NX = 4
COLS_PER_STEP = 8


def tile_at(table, tiles, r, c):
    slot = table[r * NC + c]
    return tiles[jnp.maximum(slot, 0)] * jnp.where(slot >= 0, 1.0, 0.0).astype(bf16)


def forward_kernel(extra, table, tiles, x, out):
    if extra:
        out[:, T:TALL, :] = jnp.broadcast_to(
            three_parts(sum_of_parts(x, NC)).astype(out.dtype)[None], (NX, EXTRA, T)
        )
    rows = [
        jnp.concatenate([tile_at(table, tiles, k, c) for c in range(NC)], axis=1) for k in range(NX)
    ]
    product = jnp.dot(jnp.concatenate(rows, axis=0), x[:, :T, :].reshape(NC * T, T), preferred_element_type=f32)
    out[:, :T, :] = product.astype(out.dtype).reshape(NX, T, T)


def backward_kernel(extra, table, tiles, mine, other, out):
    if extra:
        total = sum_of_parts(mine, NX) + sum_of_parts(other, NX)
        out[:, T:TALL, :] = jnp.broadcast_to(three_parts(total)[None], (NC, EXTRA, T))

    def step(i, carry):
        left = jnp.concatenate([ref[k, :T, :] for ref in (mine, other) for k in range(NX)], axis=1)
        cols = [
            jnp.concatenate([tile_at(table, tiles, r, i * COLS_PER_STEP + k) for r in range(NR)], axis=0)
            for k in range(COLS_PER_STEP)
        ]
        product = jnp.dot(left, jnp.concatenate(cols, axis=1), preferred_element_type=f32).astype(bf16)
        for k in range(COLS_PER_STEP):
            out[i * COLS_PER_STEP + k, :T, :] = product[:, k * T : (k + 1) * T]
        return carry

    lax.fori_loop(0, NC // COLS_PER_STEP, step, 0)


def multiply(kernel, table, tiles, pieces, out, extra):
    outs, kind = out
    tall = TALL if extra else T
    return pl.pallas_call(
        lambda *refs: kernel(extra, *refs),
        out_shape=jax.ShapeDtypeStruct((outs, tall, T), kind),
        in_specs=[SMEM, VMEM] + [VMEM] * len(pieces),
        out_specs=VMEM,
        cost_estimate=pl.CostEstimate(flops=2 * NR * NC * T**3, bytes_accessed=NR * NC * T * T * 2, transcendentals=0),
        compiler_params=pltpu.CompilerParams(vmem_limit_bytes=24 * MIB),
        name=kernel.__name__,
    )(table, tiles, *pieces)


def join_kernel(extra, mine, other, out):
    out[:, :T, :] = (mine[:, :T, :] + other[:, :T, :]).astype(bf16)
    if extra:
        def whole(ref):
            return jnp.sum(ref[0, T:TALL, :], axis=0, keepdims=True)

        out[:, T:TALL, :] = jnp.broadcast_to(three_parts(whole(mine) + whole(other))[None], (NX, EXTRA, T))


def block_sum(ref, count):
    total = ref[0, :T, :].astype(f32)
    for k in range(1, count):
        total = total + ref[k, :T, :].astype(f32)
    return total


def spread(out, block, row=None):
    for k in range(out.shape[0]):
        out[k, :T, :] = block
        if row is not None:
            out[k, T:TALL, :] = row


def primal_one_kernel(pieces, x, cost, low, high, step, primal, ahead):
    grad = block_sum(pieces, NC).T
    one = jnp.clip(x[...] - step[...] * (cost[...] - grad), low[...], high[...])
    primal[...] = one
    diff = one - x[...]
    spread(ahead, (2.0 * one - x[...]).astype(bf16), three_parts(jnp.sum(diff * diff, axis=0, keepdims=True)))


def dual_one_kernel(pieces, y, side, step, dual, moved, flipped):
    image = block_sum(pieces, NX)
    moved[...] = sum_of_parts(pieces, NX)
    one = jnp.maximum(y[...] + step[...] * (side[...] - image), 0.0)
    dual[...] = one
    diff = one - y[...]
    spread(flipped, one.T.astype(bf16), three_parts(jnp.sum(diff * diff, axis=0, keepdims=True)))


def primal_two_kernel(rows, cols, pieces, moved, one, cost, low, high, step, primal, weight, ahead):
    grad = block_sum(pieces, NC).T
    move_dual = sum_of_parts(pieces, NC)
    w = jnp.sqrt((move_dual / rows + EPS) / (moved[...] / cols + EPS))
    weight[...] = w
    two = jnp.clip(one[...] - step[...] / w * (cost[...] - grad), low[...], high[...])
    primal[...] = two
    spread(ahead, (2.0 * two - one[...]).astype(bf16))


def dual_two_kernel(pieces, one, side, step, weight, dual):
    image = block_sum(pieces, NX)
    dual[...] = jnp.maximum(one[...] + step[...] * weight[...] * (side[...] - image), 0.0)


def flip_kernel(y, flipped):
    spread(flipped, y[...].T.astype(bf16))


def call(kernel, outs, *args, name):
    return pl.pallas_call(
        kernel,
        out_shape=[jax.ShapeDtypeStruct(shape, kind) for shape, kind in outs],
        in_specs=[VMEM] * len(args),
        out_specs=[VMEM] * len(outs),
        compiler_params=pltpu.CompilerParams(vmem_limit_bytes=10 * MIB),
        name=name,
    )(*args)


def exchange(pieces, axis):
    return lax.all_to_all(pieces, axis, 0, 0, tiled=True)


def other_core(value):
    return lax.ppermute(value, "col_1", [(0, 1), (1, 0)])


def body(
    matrix_tiles,
    tile_rows,
    tile_cols,
    tile_count,
    x_start,
    y_start,
    cost_vector,
    right_side,
    lower_bound,
    upper_bound,
    step_primal,
    step_dual,
):
    tiles = matrix_tiles[0, 0]
    slots = tiles.shape[0]
    slot = jnp.arange(slots, dtype=jnp.int32)
    place = jnp.where(slot < tile_count[0, 0], tile_rows[0, 0] * NC + tile_cols[0, 0], -1)
    core = lax.axis_index("col_1")

    def table_of(core):
        k = jnp.arange(NR * NC, dtype=jnp.int32)
        r = k // NC
        row = (r % NX) * 2 + jnp.where(r < NX, core, 1 - core)
        wanted = row * NC + k % NC
        return jnp.max(jnp.where(place[None, :] == wanted[:, None], slot[None, :], -1), axis=1)

    table, far_table = table_of(core), table_of(1 - core)
    everyone = lax.axis_size(ROW) * lax.axis_size(COL)
    total_cols = x_start.shape[0] * everyone
    total_rows = y_start.shape[0] * everyone
    step_p, step_d = step_primal[None], step_dual[None]
    square = ((T, T), f32)
    line = ((1, T), f32)

    def to_columns(flipped, extra):
        mine = exchange(flipped, "col_0")
        pieces = (mine, other_core(mine))
        return exchange(multiply(backward_kernel, table, tiles, pieces, (NC, bf16), extra), ROW)

    def to_rows(ahead, extra):
        pieces = (exchange(ahead, ROW),)
        other = other_core(multiply(forward_kernel, far_table, tiles, pieces, (NX, f32), extra))
        mine = multiply(forward_kernel, table, tiles, pieces, (NX, f32), extra)
        tall = TALL if extra else T
        (joined,) = call(lambda *refs: join_kernel(extra, *refs), [((NX, tall, T), bf16)], mine, other, name="join")
        return exchange(joined, "col_0")

    (flipped,) = call(flip_kernel, [((NX, T, T), bf16)], y_start, name="flip")
    grads = to_columns(flipped, False)
    one, ahead = call(
        primal_one_kernel,
        [square, ((NC, TALL, T), bf16)],
        grads, x_start, cost_vector, lower_bound, upper_bound, step_p,
        name="primal_one",
    )
    images = to_rows(ahead, True)
    dual, moved, flipped = call(
        dual_one_kernel,
        [square, line, ((NX, TALL, T), bf16)],
        images, y_start, right_side, step_d,
        name="dual_one",
    )
    grads = to_columns(flipped, True)
    two, weight, ahead = call(
        lambda *refs: primal_two_kernel(float(total_rows), float(total_cols), *refs),
        [square, line, ((NC, T, T), bf16)],
        grads, moved, one, cost_vector, lower_bound, upper_bound, step_p,
        name="primal_two",
    )
    images = to_rows(ahead, False)
    (dual_out,) = call(dual_two_kernel, [square], images, dual, right_side, step_d, weight, name="dual_two")
    return (two, dual_out)


def solution(mesh):
    torus = Mesh(mesh.devices.reshape(4, 4, 4, 2), ("row_0", "row_1", "col_0", "col_1"))
    in_specs = (
        P(ROW, COL, None, None, None),
        P(ROW, COL, None),
        P(ROW, COL, None),
        P(ROW, COL),
        P(COL_ROW, None),
        P(ROW_COL, None),
        P(COL_ROW, None),
        P(ROW_COL, None),
        P(COL_ROW, None),
        P(COL_ROW, None),
        P(),
        P(),
    )
    out_specs = (P(COL_ROW, None), P(ROW_COL, None))
    return jax.shard_map(body, mesh=torus, in_specs=in_specs, out_specs=out_specs, check_vma=False)
```

```python
import jax
import jax.numpy as jnp
from jax import lax
from jax.experimental import pallas as pl
from jax.experimental.pallas import tpu as pltpu
from jax.sharding import Mesh
from jax.sharding import PartitionSpec as P

ROW = ("row_0", "row_1")
COL = ("col_0", "col_1")
ROW_COL = ("row_0", "row_1", "col_0", "col_1")
COL_ROW = ("col_0", "col_1", "row_0", "row_1")

NR = 8
NC = 16
T = 256
EXTRA = 16
TALL = T + EXTRA
EPS = 1e-06
f32 = jnp.float32
bf16 = jnp.bfloat16

VMEM = pl.BlockSpec(memory_space=pltpu.VMEM)
SMEM = pl.BlockSpec(memory_space=pltpu.SMEM)
MIB = 1 << 20


def three_parts(v):
    high = v.astype(bf16)
    rest = v - high.astype(f32)
    middle = rest.astype(bf16)
    low = (rest - middle.astype(f32)).astype(bf16)
    row = lax.broadcasted_iota(jnp.int32, (EXTRA, T), 0)
    out = jnp.where(row == 0, high.astype(f32), 0.0)
    out = jnp.where(row == 1, middle.astype(f32), out)
    return jnp.where(row == 2, low.astype(f32), out).astype(bf16)


def sum_of_parts(blocks):
    total = blocks[0][T:, :].astype(f32)
    for block in blocks[1:]:
        total = total + block[T:, :].astype(f32)
    return jnp.sum(total, axis=0, keepdims=True)


def one_row(v):
    row = lax.broadcasted_iota(jnp.int32, (WIDE - T, T), 0)
    return jnp.where(row == 0, v, 0.0)


N4 = 4
WIDE = T + 8


def tile_at(table, tiles, r, c):
    slot = table[r * NC + c]
    return tiles[jnp.maximum(slot, 0)] * jnp.where(slot >= 0, 1.0, 0.0).astype(bf16)


def call(kernel, outs, *args, name, grant=10):
    return pl.pallas_call(
        kernel,
        out_shape=[jax.ShapeDtypeStruct(shape, kind) for shape, kind in outs],
        in_specs=[VMEM] * len(args),
        out_specs=[VMEM] * len(outs),
        compiler_params=pltpu.CompilerParams(vmem_limit_bytes=grant * MIB),
        name=name,
    )(*args)


def multiply(kernel, table, tiles, pieces, out, flops, name):
    return pl.pallas_call(
        kernel,
        out_shape=jax.ShapeDtypeStruct(*out),
        in_specs=[SMEM, VMEM] + [VMEM] * len(pieces),
        out_specs=VMEM,
        cost_estimate=pl.CostEstimate(flops=flops, bytes_accessed=flops // T, transcendentals=0),
        compiler_params=pltpu.CompilerParams(vmem_limit_bytes=24 * MIB),
        name=name,
    )(table, tiles, *pieces)


def forward(table, tiles, stacks, far, extra):
    def kernel(table, tiles, *refs):
        stacks, out = refs[:-1], refs[-1]
        if extra:
            total = sum_of_parts([stack.at[a] for stack in stacks for a in range(N4)])
            out[:, T:, :] = jnp.broadcast_to(one_row(total)[None], (N4, WIDE - T, T))
        first = N4 if far else 0
        left = jnp.concatenate(
            [jnp.concatenate([tile_at(table, tiles, first + k, c) for c in range(NC)], axis=1) for k in range(N4)],
            axis=0,
        )
        right = jnp.concatenate([stack[a, :T, :] for stack in stacks for a in range(N4)], axis=0)
        product = jnp.dot(left, right, preferred_element_type=f32)
        out[:, :T, :] = product.reshape(N4, T, T)

    tall = WIDE if extra else T
    return multiply(kernel, table, tiles, stacks, ((N4, tall, T), f32), N4 * NC * 2 * T**3, "forward")


def backward(table, tiles, pieces, group, extra):
    kind = bf16 if group else f32

    def kernel(table, tiles, *refs):
        pieces, out = refs[:-1], refs[-1]
        if extra:
            total = sum_of_parts(pieces)
            rows = three_parts(total) if group else one_row(total)
            out[:, T:, :] = jnp.broadcast_to(rows[None], (N4, *rows.shape))
        left = jnp.concatenate([piece[:T, :] for piece in pieces], axis=1)
        right = jnp.concatenate(
            [
                jnp.concatenate([tile_at(table, tiles, r, group * N4 + a) for r in range(NR)], axis=0)
                for a in range(N4)
            ],
            axis=1,
        )
        product = jnp.dot(left, right, preferred_element_type=f32).astype(kind)
        for a in range(N4):
            out[a, :T, :] = product[:, a * T : (a + 1) * T]

    tall = (TALL if group else WIDE) if extra else T
    return multiply(kernel, table, tiles, pieces, ((N4, tall, T), kind), N4 * NR * 2 * T**3, "backward")


def big_sum_kernel(extra, *refs):
    stacks, outs = refs[:N4], refs[N4:]
    if extra:
        total = jnp.sum(stacks[0][0, T:, :], axis=0, keepdims=True) + sum_of_parts([s.at[0] for s in stacks[1:]])
    for a in range(N4):
        block = stacks[0][a, :T, :]
        for stack in stacks[1:]:
            block = block + stack[a, :T, :].astype(f32)
        outs[a][:T, :] = block
        if extra:
            outs[a][T:, :] = one_row(total)


def join_kernel(extra, mine, other, *outs):
    if extra:
        total = jnp.sum(mine[0, T:, :] + other[0, T:, :], axis=0, keepdims=True)
    for k, out in enumerate(outs):
        out[:T, :] = (mine[k, :T, :] + other[k, :T, :]).astype(out.dtype)
        if extra:
            out[T:, :] = three_parts(total) if k else one_row(total)


def block_sum(refs):
    total = refs[0][:T, :].astype(f32)
    for ref in refs[1:]:
        total = total + ref[:T, :].astype(f32)
    return total


def stack_kernel(*refs):
    for k in range(N4):
        refs[N4][k] = refs[k][...]


def primal_one_kernel(*refs):
    grads, (x, cost, low, high, step, primal, ahead) = refs[:N4], refs[N4:]
    grad = block_sum(grads).T
    one = jnp.clip(x[...] - step[...] * (cost[...] - grad), low[...], high[...])
    primal[...] = one
    diff = one - x[...]
    ahead[:T, :] = (2.0 * one - x[...]).astype(bf16)
    ahead[T:, :] = three_parts(jnp.sum(diff * diff, axis=0, keepdims=True))


def dual_one_kernel(*refs):
    images, (y, side, step, dual, moved, flipped) = refs[:N4], refs[N4:]
    image = block_sum(images)
    moved[...] = sum_of_parts(images[:1]) + sum_of_parts(images[1:])
    one = jnp.maximum(y[...] + step[...] * (side[...] - image), 0.0)
    dual[...] = one
    diff = one - y[...]
    flipped[:T, :] = one.T.astype(bf16)
    flipped[T:, :] = three_parts(jnp.sum(diff * diff, axis=0, keepdims=True))


def primal_two_kernel(rows, cols, *refs):
    grads, (moved, one, cost, low, high, step, primal, weight, ahead) = refs[:N4], refs[N4:]
    grad = block_sum(grads).T
    move_dual = sum_of_parts(grads)
    w = jnp.sqrt((move_dual / rows + EPS) / (moved[...] / cols + EPS))
    weight[...] = w
    two = jnp.clip(one[...] - step[...] / w * (cost[...] - grad), low[...], high[...])
    primal[...] = two
    ahead[...] = (2.0 * two - one[...]).astype(bf16)


def dual_two_kernel(*refs):
    images, (one, side, step, weight, dual) = refs[:N4], refs[N4:]
    dual[...] = jnp.maximum(one[...] + step[...] * weight[...] * (side[...] - block_sum(images)), 0.0)


def flip_kernel(y, flipped):
    flipped[...] = y[...].T.astype(bf16)


def permute(value, places):
    return lax.ppermute(value, ROW_COL, [(flat(p), flat(q)) for p, q in places])


def flat(place):
    y, z, x, core = place
    return ((y * N4 + z) * N4 + x) * 2 + core


EVERYONE = [(y, z, x, core) for y in range(N4) for z in range(N4) for x in range(N4) for core in range(2)]


def along_y(p, k):
    return ((p[0] + k) % N4, *p[1:])


def along_z(p, k):
    return (p[0], (p[1] + k) % N4, *p[2:])


def to_big(value, k):
    return permute(value, [(p, along_z(p, k) if p[3] else along_y(p, k)) for p in EVERYONE])


def to_small(value, k):
    return permute(value, [(p, along_y(p, k) if p[3] else along_z(p, k)) for p in EVERYONE])


def to_x(value, k):
    return permute(value, [(p, (*p[:2], (p[2] + k) % N4, p[3])) for p in EVERYONE])


def to_other_core(value):
    return permute(value, [(p, (*p[:3], 1 - p[3])) for p in EVERYONE])


FAR_FIRST = (2, 1, 3)


def sent(values, send):
    arrived = {k: send(values[k], k) for k in FAR_FIRST}
    return [values[0]] + [arrived[k] for k in range(1, N4)]


def body(
    matrix_tiles,
    tile_rows,
    tile_cols,
    tile_count,
    x_start,
    y_start,
    cost_vector,
    right_side,
    lower_bound,
    upper_bound,
    step_primal,
    step_dual,
):
    tiles = matrix_tiles[0, 0]
    slot = jnp.arange(tiles.shape[0], dtype=jnp.int32)
    place = jnp.where(slot < tile_count[0, 0], tile_rows[0, 0] * NC + tile_cols[0, 0], -1)
    at_y, at_z, at_x, core = (lax.axis_index(name) for name in ROW_COL)

    def table_of(sign):
        k = jnp.arange(NR * NC, dtype=jnp.int32)
        r, big, small = k // NC, k % NC // N4, k % N4
        row = (at_x + sign * r) % N4 * 2 + jnp.where(r < N4, core, 1 - core)
        y = (at_y - sign * jnp.where(core == 0, big, small)) % N4
        z = (at_z - sign * jnp.where(core == 0, small, big)) % N4
        wanted = row * NC + y * N4 + z
        return jnp.max(jnp.where(place[None, :] == wanted[:, None], slot[None, :], -1), axis=1)

    forward_table, backward_table = table_of(1), table_of(-1)
    everyone = lax.axis_size(ROW) * lax.axis_size(COL)
    total_cols = x_start.shape[0] * everyone
    total_rows = y_start.shape[0] * everyone
    step_p, step_d = step_primal[None], step_dual[None]
    square = ((T, T), f32)
    line = ((1, T), f32)

    def to_columns(flipped, extra):
        mine = sent([flipped] * N4, to_x)
        pieces = mine + [to_other_core(piece) for piece in mine]
        stacks = {k: backward(backward_table, tiles, pieces, k, extra) for k in (2, 1, 3, 0)}
        stacks = sent([stacks[k] for k in range(N4)], to_big)
        tall = WIDE if extra else T
        blocks = call(
            lambda *refs: big_sum_kernel(extra, *refs), [((tall, T), f32)] * N4, *stacks, name="big_sum"
        )
        return sent(blocks, to_small)

    def to_rows(ahead, extra):
        tall = TALL if extra else T
        (stack,) = call(
            stack_kernel, [((N4, tall, T), bf16)], *sent([ahead] * N4, to_small), name="stack"
        )
        stacks = sent([stack] * N4, to_big)
        other = to_other_core(forward(forward_table, tiles, stacks, True, extra))
        mine = forward(forward_table, tiles, stacks, False, extra)
        outs = [((WIDE if extra else T, T), f32)] + [((tall, T), bf16)] * (N4 - 1)
        blocks = call(lambda *refs: join_kernel(extra, *refs), outs, mine, other, name="join")
        return sent(blocks, to_x)

    (flipped,) = call(flip_kernel, [((T, T), bf16)], y_start, name="flip")
    grads = to_columns(flipped, False)
    one, ahead = call(
        primal_one_kernel,
        [square, ((TALL, T), bf16)],
        *grads, x_start, cost_vector, lower_bound, upper_bound, step_p,
        name="primal_one",
    )
    images = to_rows(ahead, True)
    dual, moved, flipped = call(
        dual_one_kernel,
        [square, line, ((TALL, T), bf16)],
        *images, y_start, right_side, step_d,
        name="dual_one",
    )
    grads = to_columns(flipped, True)
    two, weight, ahead = call(
        lambda *refs: primal_two_kernel(float(total_rows), float(total_cols), *refs),
        [square, line, ((T, T), bf16)],
        *grads, moved, one, cost_vector, lower_bound, upper_bound, step_p,
        name="primal_two",
    )
    images = to_rows(ahead, False)
    (dual_out,) = call(dual_two_kernel, [square], *images, dual, right_side, step_d, weight, name="dual_two")
    return (two, dual_out)


def solution(mesh):
    torus = Mesh(mesh.devices.reshape(4, 4, 4, 2), ("row_0", "row_1", "col_0", "col_1"))
    in_specs = (
        P(ROW, COL, None, None, None),
        P(ROW, COL, None),
        P(ROW, COL, None),
        P(ROW, COL),
        P(COL_ROW, None),
        P(ROW_COL, None),
        P(COL_ROW, None),
        P(ROW_COL, None),
        P(COL_ROW, None),
        P(COL_ROW, None),
        P(),
        P(),
    )
    out_specs = (P(COL_ROW, None), P(ROW_COL, None))
    return jax.shard_map(body, mesh=torus, in_specs=in_specs, out_specs=out_specs, check_vma=False)
```

```python
import jax
import jax.numpy as jnp
from jax import lax
from jax.experimental import pallas as pl
from jax.experimental.pallas import tpu as pltpu
from jax.sharding import Mesh
from jax.sharding import PartitionSpec as P


ROW = ("row_0", "row_1")
COL = ("col_0", "col_1")
ROW_COL = ("row_0", "row_1", "col_0", "col_1")
COL_ROW = ("col_0", "col_1", "row_0", "row_1")

NR = 8
NC = 16
T = 256
EXTRA = 16
TALL = T + EXTRA
EPS = 1e-06
f32 = jnp.float32
bf16 = jnp.bfloat16

VMEM = pl.BlockSpec(memory_space=pltpu.VMEM)
SMEM = pl.BlockSpec(memory_space=pltpu.SMEM)
MIB = 1 << 20


def three_parts(v):
    high = v.astype(bf16)
    rest = v - high.astype(f32)
    middle = rest.astype(bf16)
    low = (rest - middle.astype(f32)).astype(bf16)
    row = lax.broadcasted_iota(jnp.int32, (EXTRA, T), 0)
    out = jnp.where(row == 0, high.astype(f32), 0.0)
    out = jnp.where(row == 1, middle.astype(f32), out)
    return jnp.where(row == 2, low.astype(f32), out).astype(bf16)


def sum_of_parts(blocks, height=T):
    total = blocks[0][height:, :].astype(f32)
    for block in blocks[1:]:
        total = total + block[height:, :].astype(f32)
    return jnp.sum(total, axis=0, keepdims=True)


def one_row(v):
    row = lax.broadcasted_iota(jnp.int32, (WIDE - T, T), 0)
    return jnp.where(row == 0, v, 0.0)


N4 = 4
WIDE = T + 8
REST = (N4 - 1) * T


def dense_kernel(rows, cols, count, tiles, dense, table):
    at_y, at_z, at_x, core = (lax.axis_index(name) for name in ROW_COL)

    def clear(k, carry):
        table[k] = -1
        return carry

    def note(slot, carry):
        row, col = rows[0, 0, slot], cols[0, 0, slot]
        r = ((row // 2 - at_x) & 3) + jnp.where((row & 1) == core, 0, N4)
        y, z = (col // N4 - at_y) & 3, (col - at_z) & 3
        big, small = jnp.where(core == 0, y, z), jnp.where(core == 0, z, y)
        table[r * NC + big * N4 + small] = slot
        return carry

    def move(k, carry):
        slot = table[k]
        dense[k] = tiles[0, 0, jnp.maximum(slot, 0)] * jnp.where(slot >= 0, 1.0, 0.0).astype(bf16)
        return carry

    lax.fori_loop(0, NR * NC, clear, 0)
    lax.fori_loop(0, count[0, 0], note, 0)
    lax.fori_loop(0, NR * NC, move, 0)


def make_dense(rows, cols, count, tiles):
    return pl.pallas_call(
        dense_kernel,
        out_shape=jax.ShapeDtypeStruct((NR * NC, T, T), bf16),
        in_specs=[SMEM, SMEM, SMEM, VMEM],
        out_specs=VMEM,
        scratch_shapes=[pltpu.SMEM((NR * NC,), jnp.int32)],
        compiler_params=pltpu.CompilerParams(vmem_limit_bytes=4 * MIB),
        name="dense",
    )(rows, cols, count, tiles)


def call(kernel, outs, *args, grant=10):
    return pl.pallas_call(
        kernel,
        out_shape=[jax.ShapeDtypeStruct(shape, kind) for shape, kind in outs],
        in_specs=[VMEM] * len(args),
        out_specs=[VMEM] * len(outs),
        compiler_params=pltpu.CompilerParams(vmem_limit_bytes=grant * MIB),
    )(*args)


def multiply(kernel, dense, pieces, outs, tiles):
    return pl.pallas_call(
        kernel,
        out_shape=[jax.ShapeDtypeStruct(*out) for out in outs],
        in_specs=[VMEM] * (1 + len(pieces)),
        out_specs=[VMEM] * len(outs),
        cost_estimate=pl.CostEstimate(flops=tiles * 2 * T**3, bytes_accessed=tiles * 2 * T * T, transcendentals=0),
        compiler_params=pltpu.CompilerParams(vmem_limit_bytes=16 * MIB),
    )(dense, *pieces)


def back(k):
    return -k % N4


def forward(dense, near, firsts, rests, far, extra):
    def kernel(dense, *refs):
        near, firsts, rests, out = refs[:N4], refs[N4 : 2 * N4 - 1], refs[2 * N4 - 1 : -1], refs[-1]
        if extra:
            total = sum_of_parts(near) + sum_of_parts(rests, REST)
            out[:, T:, :] = jnp.broadcast_to(one_row(total)[None], (N4, WIDE - T, T))
        first = N4 if far else 0
        places = [back(b) * N4 + back(a) for b in range(N4) for a in range(N4)]
        left = jnp.concatenate(
            [jnp.concatenate([dense[(first + k) * NC + c] for c in places], axis=1) for k in range(N4)], axis=0
        )
        right = [tile[:T, :] for tile in near]
        for one, rest in zip(firsts, rests):
            right += [one[:T, :], rest[:REST, :]]
        product = jnp.dot(left, jnp.concatenate(right, axis=0), preferred_element_type=f32)
        out[:, :T, :] = product.reshape(N4, T, T)

    tall = WIDE if extra else T
    outs = [((N4, tall, T), f32)]
    return multiply(kernel, dense, [*near, *firsts, *rests], outs, N4 * NC)[0]


def transposed_product(dense, pieces, places):
    left = jnp.concatenate([piece[:T, :] for piece in pieces], axis=1)
    rows = [first + back(k) for first in (0, N4) for k in range(N4)]
    right = jnp.concatenate(
        [jnp.concatenate([dense[r * NC + c] for r in rows], axis=0) for c in places], axis=1
    )
    product = jnp.dot(left, right, preferred_element_type=f32)
    return [product[:, k * T : (k + 1) * T] for k in range(len(places))]


def backward_rest(dense, pieces, group, extra):
    def kernel(dense, *refs):
        pieces, out = refs[:-1], refs[-1]
        if extra:
            out[REST:, :] = three_parts(sum_of_parts(pieces))
        for a, block in enumerate(transposed_product(dense, pieces, range(group * N4 + 1, group * N4 + N4))):
            out[a * T : (a + 1) * T, :] = block.astype(bf16)

    outs = [((REST + (EXTRA if extra else 0), T), bf16)]
    return multiply(kernel, dense, pieces, outs, (N4 - 1) * NR)[0]


def backward_near(dense, pieces, extra):
    def kernel(dense, *refs):
        pieces, (own, rest, moved), firsts = refs[: 2 * N4], refs[2 * N4 : 2 * N4 + 3], refs[2 * N4 + 3 :]
        moved[...] = sum_of_parts(pieces) if extra else jnp.zeros((1, T), f32)
        blocks = transposed_product(dense, pieces, [0, 1, 2, 3, 4, 8, 12])
        own[...] = blocks[0]
        for a in range(1, N4):
            rest[(a - 1) * T : a * T, :] = blocks[a]
        for out, block in zip(firsts, blocks[N4:]):
            out[...] = block.astype(bf16)

    outs = [((T, T), f32), ((REST, T), f32), ((1, T), f32)] + [((T, T), bf16)] * (N4 - 1)
    own, rest, moved, *firsts = multiply(kernel, dense, pieces, outs, 7 * NR)
    return own, rest, moved, firsts


def big_sum_kernel(extra, own, own_moved, *refs):
    rests, outs, moved = refs[: N4 - 1], refs[N4 - 1 : -1], refs[-1]
    total = own_moved[...]
    if extra:
        total = total + sum_of_parts(rests, REST)
    moved[...] = total
    for a, out in enumerate(outs):
        block = own[a * T : (a + 1) * T, :]
        for rest in rests:
            block = block + rest[a * T : (a + 1) * T, :].astype(f32)
        out[:T, :] = block
        if extra:
            out[T:, :] = one_row(total)


def join_kernel(extra, mine, other, *outs):
    if extra:
        total = jnp.sum(mine[0, T:, :] + other[0, T:, :], axis=0, keepdims=True)
    for k, out in enumerate(outs):
        out[:T, :] = (mine[k, :T, :] + other[k, :T, :]).astype(out.dtype)
        if extra:
            out[T:, :] = three_parts(total) if k else one_row(total)


def block_sum(refs):
    total = refs[0][:T, :].astype(f32)
    for ref in refs[1:]:
        total = total + ref[:T, :].astype(f32)
    return total


def rest_kernel(extra, *refs):
    near, out = refs[:N4], refs[N4]
    for a in range(1, N4):
        out[(a - 1) * T : a * T, :] = near[a][:T, :]
    if extra:
        out[REST:, :] = three_parts(sum_of_parts(near))


BLOCKS = 2 * N4 - 1


def primal_one_kernel(*refs):
    grads, (x, cost, low, high, step, primal, ahead) = refs[:BLOCKS], refs[BLOCKS:]
    grad = block_sum(grads).T
    one = jnp.clip(x[...] - step[...] * (cost[...] - grad), low[...], high[...])
    primal[...] = one
    diff = one - x[...]
    ahead[:T, :] = (2.0 * one - x[...]).astype(bf16)
    ahead[T:, :] = three_parts(jnp.sum(diff * diff, axis=0, keepdims=True))


def dual_one_kernel(*refs):
    images, (y, side, step, dual, moved, flipped) = refs[:N4], refs[N4:]
    image = block_sum(images)
    moved[...] = sum_of_parts(images[:1]) + sum_of_parts(images[1:])
    one = jnp.maximum(y[...] + step[...] * (side[...] - image), 0.0)
    dual[...] = one
    diff = one - y[...]
    flipped[:T, :] = one.T.astype(bf16)
    flipped[T:, :] = three_parts(jnp.sum(diff * diff, axis=0, keepdims=True))


def primal_two_kernel(rows, cols, *refs):
    grads = refs[:BLOCKS]
    line, moved, one, cost, low, high, step, primal, weight, ahead = refs[BLOCKS:]
    grad = block_sum(grads).T
    move_dual = line[...] + sum_of_parts(grads[N4:])
    w = jnp.sqrt((move_dual / rows + EPS) / (moved[...] / cols + EPS))
    weight[...] = w
    two = jnp.clip(one[...] - step[...] / w * (cost[...] - grad), low[...], high[...])
    primal[...] = two
    ahead[...] = (2.0 * two - one[...]).astype(bf16)


def dual_two_kernel(*refs):
    images, (one, side, step, weight, dual) = refs[:N4], refs[N4:]
    dual[...] = jnp.maximum(one[...] + step[...] * weight[...] * (side[...] - block_sum(images)), 0.0)


def flip_kernel(y, flipped):
    flipped[...] = y[...].T.astype(bf16)


def permute(value, places):
    return lax.ppermute(value, ROW_COL, [(flat(p), flat(q)) for p, q in places])


def flat(place):
    y, z, x, core = place
    return ((y * N4 + z) * N4 + x) * 2 + core


EVERYONE = [(y, z, x, core) for y in range(N4) for z in range(N4) for x in range(N4) for core in range(2)]


def along_y(p, k):
    return ((p[0] + k) % N4, *p[1:])


def along_z(p, k):
    return (p[0], (p[1] + k) % N4, *p[2:])


def to_big(value, k):
    return permute(value, [(p, along_z(p, k) if p[3] else along_y(p, k)) for p in EVERYONE])


def to_small(value, k):
    return permute(value, [(p, along_y(p, k) if p[3] else along_z(p, k)) for p in EVERYONE])


def to_x(value, k):
    return permute(value, [(p, (*p[:2], (p[2] + k) % N4, p[3])) for p in EVERYONE])


def to_other_core(value):
    return permute(value, [(p, (*p[:3], 1 - p[3])) for p in EVERYONE])


FAR_FIRST = (2, 1, 3)


def sent(values, send):
    arrived = {k: send(values[k - 1], k) for k in FAR_FIRST}
    return [arrived[k] for k in range(1, N4)]


def body(
    matrix_tiles,
    tile_rows,
    tile_cols,
    tile_count,
    x_start,
    y_start,
    cost_vector,
    right_side,
    lower_bound,
    upper_bound,
    step_primal,
    step_dual,
):
    dense = make_dense(tile_rows, tile_cols, tile_count, matrix_tiles)
    everyone = lax.axis_size(ROW) * lax.axis_size(COL)
    total_cols = x_start.shape[0] * everyone
    total_rows = y_start.shape[0] * everyone
    step_p, step_d = step_primal[None], step_dual[None]
    square = ((T, T), f32)
    line = ((1, T), f32)

    def to_columns(flipped, extra, ready=None):
        mine = [flipped] + sent([flipped] * 3, to_x)
        if ready is not None:
            mine[0], ready = lax.optimization_barrier((flipped, ready))
        matrix = dense if ready is None else ready
        pieces = mine + [to_other_core(piece) for piece in mine]
        rests = {k: backward_rest(matrix, pieces, k, extra) for k in FAR_FIRST}
        rests = sent([rests[k] for k in range(1, N4)], to_big)
        own, own_rest, moved, firsts = backward_near(matrix, pieces, extra)
        firsts = sent(firsts, to_big)
        tall = WIDE if extra else T
        *blocks, moved = call(
            lambda *refs: big_sum_kernel(extra, *refs), [((tall, T), f32)] * 3 + [line], own_rest, moved, *rests,
        )
        return [own, *firsts, *sent(blocks, to_small)], moved

    def to_rows(ahead, extra):
        near = [ahead] + sent([ahead] * 3, to_small)
        firsts = sent([ahead] * 3, to_big)
        tall = TALL if extra else T
        (rest,) = call(lambda *refs: rest_kernel(extra, *refs), [((REST + tall - T, T), bf16)], *near)
        rests = sent([rest] * 3, to_big)
        other = to_other_core(forward(dense, near, firsts, rests, True, extra))
        mine = forward(dense, near, firsts, rests, False, extra)
        outs = [((WIDE if extra else T, T), f32)] + [((tall, T), bf16)] * (N4 - 1)
        own, *blocks = call(lambda *refs: join_kernel(extra, *refs), outs, mine, other)
        return [own, *sent(blocks, to_x)]

    (flipped,) = call(flip_kernel, [((T, T), bf16)], y_start)
    grads, _ = to_columns(flipped, False, dense)
    one, ahead = call(
        primal_one_kernel,
        [square, ((TALL, T), bf16)],
        *grads, x_start, cost_vector, lower_bound, upper_bound, step_p,
    )
    images = to_rows(ahead, True)
    dual, moved, flipped = call(
        dual_one_kernel,
        [square, line, ((TALL, T), bf16)],
        *images, y_start, right_side, step_d,
    )
    grads, moved_line = to_columns(flipped, True)
    two, weight, ahead = call(
        lambda *refs: primal_two_kernel(float(total_rows), float(total_cols), *refs),
        [square, line, ((T, T), bf16)],
        *grads, moved_line, moved, one, cost_vector, lower_bound, upper_bound, step_p,
    )
    images = to_rows(ahead, False)
    (dual_out,) = call(dual_two_kernel, [square], *images, dual, right_side, step_d, weight)
    return (two, dual_out)


def solution(mesh):
    torus = Mesh(mesh.devices.reshape(4, 4, 4, 2), ("row_0", "row_1", "col_0", "col_1"))
    in_specs = (
        P(ROW, COL, None, None, None),
        P(ROW, COL, None),
        P(ROW, COL, None),
        P(ROW, COL),
        P(COL_ROW, None),
        P(ROW_COL, None),
        P(COL_ROW, None),
        P(ROW_COL, None),
        P(COL_ROW, None),
        P(COL_ROW, None),
        P(),
        P(),
    )
    out_specs = (P(COL_ROW, None), P(ROW_COL, None))
    return jax.shard_map(body, mesh=torus, in_specs=in_specs, out_specs=out_specs, check_vma=False)
```

```python
import jax
import jax.numpy as jnp
from jax import lax
from jax.experimental import pallas as pl
from jax.experimental.pallas import tpu as pltpu
from jax.sharding import Mesh
from jax.sharding import PartitionSpec as P


ROW = ("row_0", "row_1")
COL = ("col_0", "col_1")
ROW_COL = ("row_0", "row_1", "col_0", "col_1")
COL_ROW = ("col_0", "col_1", "row_0", "row_1")

NR = 8
NC = 16
T = 256
EXTRA = 16
TALL = T + EXTRA
EPS = 1e-06
f32 = jnp.float32
bf16 = jnp.bfloat16

VMEM = pl.BlockSpec(memory_space=pltpu.VMEM)
SMEM = pl.BlockSpec(memory_space=pltpu.SMEM)
MIB = 1 << 20


def three_parts(v):
    high = v.astype(bf16)
    rest = v - high.astype(f32)
    middle = rest.astype(bf16)
    low = (rest - middle.astype(f32)).astype(bf16)
    row = lax.broadcasted_iota(jnp.int32, (EXTRA, T), 0)
    out = jnp.where(row == 0, high.astype(f32), 0.0)
    out = jnp.where(row == 1, middle.astype(f32), out)
    return jnp.where(row == 2, low.astype(f32), out).astype(bf16)


def sum_of_parts(blocks, height=T):
    total = blocks[0][height:, :].astype(f32)
    for block in blocks[1:]:
        total = total + block[height:, :].astype(f32)
    return jnp.sum(total, axis=0, keepdims=True)


def one_row(v):
    row = lax.broadcasted_iota(jnp.int32, (WIDE - T, T), 0)
    return jnp.where(row == 0, v, 0.0)


N4 = 4
WIDE = T + 8
REST = (N4 - 1) * T


def dense_kernel(rows, cols, count, tiles, dense, table):
    at_y, at_z, at_x, core = (lax.axis_index(name) for name in ROW_COL)

    used = count[0, 0]

    def clear(k, carry):
        table[k] = -1
        return carry

    def note(slot, carry):
        row, col = rows[0, 0, slot], cols[0, 0, slot]
        r = ((lax.shift_right_logical(row, 1) - at_x) & 3) + jnp.where((row & 1) == core, 0, N4)
        y, z = (lax.shift_right_logical(col, 2) - at_y) & 3, (col - at_z) & 3
        place = r * NC + jnp.where(core == 1, y * N4 + z, z * N4 + y)
        table[jnp.where(slot < used, place, NR * NC)] = slot
        return carry

    def move(k, carry):
        slot = table[k]
        dense[k] = tiles[0, 0, jnp.maximum(slot, 0)] * jnp.where(slot >= 0, 1.0, 0.0).astype(bf16)
        return carry

    lax.fori_loop(0, NR * NC, clear, 0, unroll=16)
    lax.fori_loop(0, tiles.shape[2], note, 0, unroll=8)
    lax.fori_loop(0, NR * NC, move, 0, unroll=4)


def make_dense(rows, cols, count, tiles):
    return pl.pallas_call(
        dense_kernel,
        out_shape=jax.ShapeDtypeStruct((NR * NC, T, T), bf16),
        in_specs=[SMEM, SMEM, SMEM, VMEM],
        out_specs=VMEM,
        scratch_shapes=[pltpu.SMEM((NR * NC + 8,), jnp.int32)],
        compiler_params=pltpu.CompilerParams(vmem_limit_bytes=4 * MIB),
        name="dense",
    )(rows, cols, count, tiles)


def call(kernel, outs, *args, grant=10):
    return pl.pallas_call(
        kernel,
        out_shape=[jax.ShapeDtypeStruct(shape, kind) for shape, kind in outs],
        in_specs=[VMEM] * len(args),
        out_specs=[VMEM] * len(outs),
        compiler_params=pltpu.CompilerParams(vmem_limit_bytes=grant * MIB),
    )(*args)


def multiply(kernel, dense, pieces, outs, tiles):
    return pl.pallas_call(
        kernel,
        out_shape=[jax.ShapeDtypeStruct(*out) for out in outs],
        in_specs=[VMEM] * (1 + len(pieces)),
        out_specs=[VMEM] * len(outs),
        cost_estimate=pl.CostEstimate(flops=tiles * 2 * T**3, bytes_accessed=tiles * 2 * T * T, transcendentals=0),
        compiler_params=pltpu.CompilerParams(vmem_limit_bytes=16 * MIB),
    )(dense, *pieces)


def back(k):
    return -k % N4


def tile_rows_of(dense, rows, places):
    return jnp.concatenate(
        [jnp.concatenate([dense[r * NC + c] for c in places], axis=1) for r in rows], axis=0
    )


def forward_early(dense, near, firsts):
    def kernel(dense, *refs):
        pieces, out = refs[:-1], refs[-1]
        places = [back(a) for a in range(N4)] + [back(b) * N4 for b in range(1, N4)]
        right = jnp.concatenate([piece[:T, :] for piece in pieces], axis=0)
        for half in range(2):
            rows = range(half * N4, half * N4 + N4)
            product = jnp.dot(tile_rows_of(dense, rows, places), right, preferred_element_type=f32)
            out[half * N4 : half * N4 + N4] = product.reshape(N4, T, T)

    return multiply(kernel, dense, [*near, *firsts], [((NR, T, T), f32)], 7 * NR)[0]


def forward_late(dense, early, near, rests, far, extra):
    def kernel(dense, *refs):
        early, near, rests, out = refs[0], refs[1 : 1 + N4], refs[1 + N4 : -1], refs[-1]
        if extra:
            total = sum_of_parts(near) + sum_of_parts(rests, REST)
            out[:, T:, :] = jnp.broadcast_to(one_row(total)[None], (N4, WIDE - T, T))
        first = N4 if far else 0
        places = [back(b) * N4 + back(a) for b in range(1, N4) for a in range(1, N4)]
        left = tile_rows_of(dense, range(first, first + N4), places)
        right = jnp.concatenate([rest[:REST, :] for rest in rests], axis=0)
        product = jnp.dot(left, right, preferred_element_type=f32)
        out[:, :T, :] = product.reshape(N4, T, T) + early[first : first + N4]

    outs = [((N4, WIDE if extra else T, T), f32)]
    return multiply(kernel, dense, [early, *near, *rests], outs, 9 * N4)[0]


def transposed_product(dense, pieces, places):
    left = jnp.concatenate([piece[:T, :] for piece in pieces], axis=1)
    rows = [first + back(k) for first in (0, N4) for k in range(N4)]
    right = jnp.concatenate(
        [jnp.concatenate([dense[r * NC + c] for r in rows], axis=0) for c in places], axis=1
    )
    product = jnp.dot(left, right, preferred_element_type=f32)
    return [product[:, k * T : (k + 1) * T] for k in range(len(places))]


def backward_rest(dense, pieces, group, extra):
    def kernel(dense, *refs):
        pieces, out = refs[:-1], refs[-1]
        if extra:
            out[REST:, :] = three_parts(sum_of_parts(pieces))
        for a, block in enumerate(transposed_product(dense, pieces, range(group * N4 + 1, group * N4 + N4))):
            out[a * T : (a + 1) * T, :] = block.astype(bf16)

    outs = [((REST + (EXTRA if extra else 0), T), bf16)]
    return multiply(kernel, dense, pieces, outs, (N4 - 1) * NR)[0]


def backward_near(dense, pieces, extra):
    def kernel(dense, *refs):
        pieces, (own, rest, moved), firsts = refs[: 2 * N4], refs[2 * N4 : 2 * N4 + 3], refs[2 * N4 + 3 :]
        moved[...] = sum_of_parts(pieces) if extra else jnp.zeros((1, T), f32)
        blocks = transposed_product(dense, pieces, [0, 1, 2, 3, 4, 8, 12])
        own[...] = blocks[0]
        for a in range(1, N4):
            rest[(a - 1) * T : a * T, :] = blocks[a]
        for out, block in zip(firsts, blocks[N4:]):
            out[...] = block.astype(bf16)

    outs = [((T, T), f32), ((REST, T), f32), ((1, T), f32)] + [((T, T), bf16)] * (N4 - 1)
    own, rest, moved, *firsts = multiply(kernel, dense, pieces, outs, 7 * NR)
    return own, rest, moved, firsts


def big_sum_kernel(extra, own, own_moved, *refs):
    rests, outs, moved = refs[: N4 - 1], refs[N4 - 1 : -1], refs[-1]
    total = own_moved[...]
    if extra:
        total = total + sum_of_parts(rests, REST)
    moved[...] = total
    for a, out in enumerate(outs):
        block = own[a * T : (a + 1) * T, :]
        for rest in rests:
            block = block + rest[a * T : (a + 1) * T, :].astype(f32)
        out[:T, :] = block
        if extra:
            out[T:, :] = one_row(total)


def join_kernel(extra, mine, other, *outs):
    if extra:
        total = jnp.sum(mine[0, T:, :] + other[0, T:, :], axis=0, keepdims=True)
    for k, out in enumerate(outs):
        out[:T, :] = (mine[k, :T, :] + other[k, :T, :]).astype(out.dtype)
        if extra:
            out[T:, :] = three_parts(total) if k else one_row(total)


def block_sum(refs):
    total = refs[0][:T, :].astype(f32)
    for ref in refs[1:]:
        total = total + ref[:T, :].astype(f32)
    return total


def rest_kernel(extra, *refs):
    near, out = refs[:N4], refs[N4]
    for a in range(1, N4):
        out[(a - 1) * T : a * T, :] = near[a][:T, :]
    if extra:
        out[REST:, :] = three_parts(sum_of_parts(near))


BLOCKS = 2 * N4 - 1


def primal_one_kernel(*refs):
    grads, (x, cost, low, high, step, primal, ahead) = refs[:BLOCKS], refs[BLOCKS:]
    grad = block_sum(grads).T
    one = jnp.clip(x[...] - step[...] * (cost[...] - grad), low[...], high[...])
    primal[...] = one
    diff = one - x[...]
    ahead[:T, :] = (2.0 * one - x[...]).astype(bf16)
    ahead[T:, :] = three_parts(jnp.sum(diff * diff, axis=0, keepdims=True))


def dual_one_kernel(*refs):
    images, (y, side, step, dual, moved, flipped) = refs[:N4], refs[N4:]
    image = block_sum(images)
    moved[...] = sum_of_parts(images[:1]) + sum_of_parts(images[1:])
    one = jnp.maximum(y[...] + step[...] * (side[...] - image), 0.0)
    dual[...] = one
    diff = one - y[...]
    flipped[:T, :] = one.T.astype(bf16)
    flipped[T:, :] = three_parts(jnp.sum(diff * diff, axis=0, keepdims=True))


def primal_two_kernel(rows, cols, *refs):
    grads = refs[:BLOCKS]
    line, moved, one, cost, low, high, step, primal, weight, ahead = refs[BLOCKS:]
    grad = block_sum(grads).T
    move_dual = line[...] + sum_of_parts(grads[N4:])
    w = jnp.sqrt((move_dual / rows + EPS) / (moved[...] / cols + EPS))
    weight[...] = w
    two = jnp.clip(one[...] - step[...] / w * (cost[...] - grad), low[...], high[...])
    primal[...] = two
    ahead[...] = (2.0 * two - one[...]).astype(bf16)


def dual_two_kernel(*refs):
    images, (one, side, step, weight, dual) = refs[:N4], refs[N4:]
    dual[...] = jnp.maximum(one[...] + step[...] * weight[...] * (side[...] - block_sum(images)), 0.0)


def flip_kernel(y, flipped):
    flipped[...] = y[...].T.astype(bf16)


def permute(value, places):
    return lax.ppermute(value, ROW_COL, [(flat(p), flat(q)) for p, q in places])


def flat(place):
    y, z, x, core = place
    return ((y * N4 + z) * N4 + x) * 2 + core


EVERYONE = [(y, z, x, core) for y in range(N4) for z in range(N4) for x in range(N4) for core in range(2)]


def along_y(p, k):
    return ((p[0] + k) % N4, *p[1:])


def along_z(p, k):
    return (p[0], (p[1] + k) % N4, *p[2:])


def to_big(value, k):
    return permute(value, [(p, along_y(p, k) if p[3] else along_z(p, k)) for p in EVERYONE])


def to_small(value, k):
    return permute(value, [(p, along_z(p, k) if p[3] else along_y(p, k)) for p in EVERYONE])


def to_x(value, k):
    return permute(value, [(p, (*p[:2], (p[2] + k) % N4, p[3])) for p in EVERYONE])


def to_other_core(value):
    return permute(value, [(p, (*p[:3], 1 - p[3])) for p in EVERYONE])


FAR_FIRST = (1, 3, 2)


START_ORDER = (1, 3, 2)


def sent(values, send):
    arrived = {}
    for k in START_ORDER:
        arrived[k] = send(values[k - 1], k)
    return [arrived[k] for k in range(1, N4)]


def body(
    matrix_tiles,
    tile_rows,
    tile_cols,
    tile_count,
    x_start,
    y_start,
    cost_vector,
    right_side,
    lower_bound,
    upper_bound,
    step_primal,
    step_dual,
):
    dense = make_dense(tile_rows, tile_cols, tile_count, matrix_tiles)
    everyone = lax.axis_size(ROW) * lax.axis_size(COL)
    total_cols = x_start.shape[0] * everyone
    total_rows = y_start.shape[0] * everyone
    step_p, step_d = step_primal[None], step_dual[None]
    square = ((T, T), f32)
    line = ((1, T), f32)

    def to_columns(flipped, extra, ready=None):
        mine = [flipped] + sent([flipped] * 3, to_x)
        if ready is not None:
            mine[0], ready = lax.optimization_barrier((flipped, ready))
        matrix = dense if ready is None else ready
        pieces = mine + [to_other_core(piece) for piece in mine]
        rests = {k: backward_rest(matrix, pieces, k, extra) for k in FAR_FIRST}
        rests = sent([rests[k] for k in range(1, N4)], to_big)
        own, own_rest, moved, firsts = backward_near(matrix, pieces, extra)
        firsts = sent(firsts, to_big)
        tall = WIDE if extra else T
        *blocks, moved = call(
            lambda *refs: big_sum_kernel(extra, *refs), [((tall, T), f32)] * 3 + [line], own_rest, moved, *rests,
        )
        return [own, *firsts, *sent(blocks, to_small)], moved

    def to_rows(ahead, extra):
        near = [ahead] + sent([ahead] * 3, to_small)
        firsts = sent([ahead] * 3, to_big)
        tall = TALL if extra else T
        (rest,) = call(lambda *refs: rest_kernel(extra, *refs), [((REST + tall - T, T), bf16)], *near)
        rests = sent([rest] * 3, to_big)
        early = forward_early(dense, near, firsts)
        other = to_other_core(forward_late(dense, early, near, rests, True, extra))
        mine = forward_late(dense, early, near, rests, False, extra)
        outs = [((WIDE if extra else T, T), f32)] + [((tall, T), bf16)] * (N4 - 1)
        own, *blocks = call(lambda *refs: join_kernel(extra, *refs), outs, mine, other)
        return [own, *sent(blocks, to_x)]

    (flipped,) = call(flip_kernel, [((T, T), bf16)], y_start)
    grads, _ = to_columns(flipped, False, dense)
    one, ahead = call(
        primal_one_kernel,
        [square, ((TALL, T), bf16)],
        *grads, x_start, cost_vector, lower_bound, upper_bound, step_p,
    )
    images = to_rows(ahead, True)
    dual, moved, flipped = call(
        dual_one_kernel,
        [square, line, ((TALL, T), bf16)],
        *images, y_start, right_side, step_d,
    )
    grads, moved_line = to_columns(flipped, True)
    two, weight, ahead = call(
        lambda *refs: primal_two_kernel(float(total_rows), float(total_cols), *refs),
        [square, line, ((T, T), bf16)],
        *grads, moved_line, moved, one, cost_vector, lower_bound, upper_bound, step_p,
    )
    images = to_rows(ahead, False)
    (dual_out,) = call(dual_two_kernel, [square], *images, dual, right_side, step_d, weight)
    return (two, dual_out)


def solution(mesh):
    torus = Mesh(mesh.devices.reshape(4, 4, 4, 2), ("row_0", "row_1", "col_0", "col_1"))
    in_specs = (
        P(ROW, COL, None, None, None),
        P(ROW, COL, None),
        P(ROW, COL, None),
        P(ROW, COL),
        P(COL_ROW, None),
        P(ROW_COL, None),
        P(COL_ROW, None),
        P(ROW_COL, None),
        P(COL_ROW, None),
        P(COL_ROW, None),
        P(),
        P(),
    )
    out_specs = (P(COL_ROW, None), P(ROW_COL, None))
    return jax.shard_map(body, mesh=torus, in_specs=in_specs, out_specs=out_specs, check_vma=False)
```

```python
import jax
import jax.numpy as jnp
from jax import lax
from jax.experimental import pallas as pl
from jax.experimental.pallas import tpu as pltpu
from jax.sharding import Mesh
from jax.sharding import PartitionSpec as P


ROW = ("row_0", "row_1")
COL = ("col_0", "col_1")
ROW_COL = ("row_0", "row_1", "col_0", "col_1")
COL_ROW = ("col_0", "col_1", "row_0", "row_1")

NR = 8
NC = 16
T = 256
EXTRA = 16
TALL = T + EXTRA
EPS = 1e-06
f32 = jnp.float32
bf16 = jnp.bfloat16

VMEM = pl.BlockSpec(memory_space=pltpu.VMEM)
SMEM = pl.BlockSpec(memory_space=pltpu.SMEM)
MIB = 1 << 20


def three_parts(v):
    high = v.astype(bf16)
    rest = v - high.astype(f32)
    middle = rest.astype(bf16)
    low = (rest - middle.astype(f32)).astype(bf16)
    row = lax.broadcasted_iota(jnp.int32, (EXTRA, T), 0)
    out = jnp.where(row == 0, high.astype(f32), 0.0)
    out = jnp.where(row == 1, middle.astype(f32), out)
    return jnp.where(row == 2, low.astype(f32), out).astype(bf16)


def sum_of_parts(blocks, height=T):
    total = blocks[0][height:, :].astype(f32)
    for block in blocks[1:]:
        total = total + block[height:, :].astype(f32)
    return jnp.sum(total, axis=0, keepdims=True)


def one_row(v):
    row = lax.broadcasted_iota(jnp.int32, (WIDE - T, T), 0)
    return jnp.where(row == 0, v, 0.0)


N4 = 4
WIDE = T + 8
REST = (N4 - 1) * T


def dense_kernel(rows, cols, count, tiles, dense, table):
    at_y, at_z, at_x, core = (lax.axis_index(name) for name in ROW_COL)

    used = count[0, 0]

    def clear(k, carry):
        table[k] = -1
        return carry

    def note(slot, carry):
        row, col = rows[0, 0, slot], cols[0, 0, slot]
        r = ((lax.shift_right_logical(row, 1) - at_x) & 3) + jnp.where((row & 1) == core, 0, N4)
        y, z = (lax.shift_right_logical(col, 2) - at_y) & 3, (col - at_z) & 3
        place = r * NC + jnp.where(core == 1, y * N4 + z, z * N4 + y)
        table[jnp.where(slot < used, place, NR * NC)] = slot
        return carry

    def move(k, carry):
        slot = table[k]
        dense[k] = tiles[0, 0, jnp.maximum(slot, 0)] * jnp.where(slot >= 0, 1.0, 0.0).astype(bf16)
        return carry

    lax.fori_loop(0, NR * NC, clear, 0, unroll=16)
    lax.fori_loop(0, tiles.shape[2], note, 0, unroll=8)
    lax.fori_loop(0, NR * NC, move, 0, unroll=4)


def make_dense(rows, cols, count, tiles):
    return pl.pallas_call(
        dense_kernel,
        out_shape=jax.ShapeDtypeStruct((NR * NC, T, T), bf16),
        in_specs=[SMEM, SMEM, SMEM, VMEM],
        out_specs=VMEM,
        scratch_shapes=[pltpu.SMEM((NR * NC + 8,), jnp.int32)],
        compiler_params=pltpu.CompilerParams(vmem_limit_bytes=4 * MIB),
        name="dense",
    )(rows, cols, count, tiles)


def call(kernel, outs, *args, grant=10):
    return pl.pallas_call(
        kernel,
        out_shape=[jax.ShapeDtypeStruct(shape, kind) for shape, kind in outs],
        in_specs=[VMEM] * len(args),
        out_specs=[VMEM] * len(outs),
        compiler_params=pltpu.CompilerParams(vmem_limit_bytes=grant * MIB),
    )(*args)


def multiply(kernel, dense, pieces, outs, tiles):
    return pl.pallas_call(
        kernel,
        out_shape=[jax.ShapeDtypeStruct(*out) for out in outs],
        in_specs=[VMEM] * (1 + len(pieces)),
        out_specs=[VMEM] * len(outs),
        cost_estimate=pl.CostEstimate(flops=tiles * 2 * T**3, bytes_accessed=tiles * 2 * T * T, transcendentals=0),
        compiler_params=pltpu.CompilerParams(vmem_limit_bytes=16 * MIB),
    )(dense, *pieces)


def back(k):
    return -k % N4


def tile_rows_of(dense, rows, places):
    return jnp.concatenate(
        [jnp.concatenate([dense[r * NC + c] for c in places], axis=1) for r in rows], axis=0
    )


def forward_early(dense, near, firsts):
    def kernel(dense, *refs):
        pieces, out = refs[:-1], refs[-1]
        places = [back(a) for a in range(N4)] + [back(b) * N4 for b in range(1, N4)]
        right = jnp.concatenate([piece[:T, :] for piece in pieces], axis=0)
        for half in range(2):
            rows = range(half * N4, half * N4 + N4)
            product = jnp.dot(tile_rows_of(dense, rows, places), right, preferred_element_type=f32)
            out[half * N4 : half * N4 + N4] = product.reshape(N4, T, T)

    return multiply(kernel, dense, [*near, *firsts], [((NR, T, T), f32)], 7 * NR)[0]


def forward_late(dense, early, near, rests, far, extra):
    def kernel(dense, *refs):
        early, near, rests, out = refs[0], refs[1 : 1 + N4], refs[1 + N4 : -1], refs[-1]
        if extra:
            total = sum_of_parts(near) + sum_of_parts(rests, REST)
            out[:, T:, :] = jnp.broadcast_to(one_row(total)[None], (N4, WIDE - T, T))
        first = N4 if far else 0
        places = [back(b) * N4 + back(a) for b in range(1, N4) for a in range(1, N4)]
        left = tile_rows_of(dense, range(first, first + N4), places)
        right = jnp.concatenate([rest[:REST, :] for rest in rests], axis=0)
        product = jnp.dot(left, right, preferred_element_type=f32)
        out[:, :T, :] = product.reshape(N4, T, T) + early[first : first + N4]

    outs = [((N4, WIDE if extra else T, T), f32)]
    return multiply(kernel, dense, [early, *near, *rests], outs, 9 * N4)[0]


def transposed_product(dense, pieces, places):
    left = jnp.concatenate([piece[:T, :] for piece in pieces], axis=1)
    rows = [first + back(k) for first in (0, N4) for k in range(N4)]
    right = jnp.concatenate(
        [jnp.concatenate([dense[r * NC + c] for r in rows], axis=0) for c in places], axis=1
    )
    product = jnp.dot(left, right, preferred_element_type=f32)
    return [product[:, k * T : (k + 1) * T] for k in range(len(places))]


def backward_rest(dense, pieces, group, extra):
    def kernel(dense, *refs):
        pieces, out = refs[:-1], refs[-1]
        if extra:
            out[REST:, :] = three_parts(sum_of_parts(pieces))
        for a, block in enumerate(transposed_product(dense, pieces, range(group * N4 + 1, group * N4 + N4))):
            out[a * T : (a + 1) * T, :] = block.astype(bf16)

    outs = [((REST + (EXTRA if extra else 0), T), bf16)]
    return multiply(kernel, dense, pieces, outs, (N4 - 1) * NR)[0]


def backward_near(dense, pieces, extra):
    def kernel(dense, *refs):
        pieces, (own, rest, moved), firsts = refs[: 2 * N4], refs[2 * N4 : 2 * N4 + 3], refs[2 * N4 + 3 :]
        moved[...] = sum_of_parts(pieces) if extra else jnp.zeros((1, T), f32)
        blocks = transposed_product(dense, pieces, [0, 1, 2, 3, 4, 8, 12])
        own[...] = blocks[0]
        for a in range(1, N4):
            rest[(a - 1) * T : a * T, :] = blocks[a]
        for out, block in zip(firsts, blocks[N4:]):
            out[...] = block.astype(bf16)

    outs = [((T, T), f32), ((REST, T), f32), ((1, T), f32)] + [((T, T), bf16)] * (N4 - 1)
    own, rest, moved, *firsts = multiply(kernel, dense, pieces, outs, 7 * NR)
    return own, rest, moved, firsts


def big_sum_kernel(extra, own, own_moved, *refs):
    rests, outs, moved = refs[: N4 - 1], refs[N4 - 1 : -1], refs[-1]
    total = own_moved[...]
    if extra:
        total = total + sum_of_parts(rests, REST)
    moved[...] = total
    for a, out in enumerate(outs):
        block = own[a * T : (a + 1) * T, :]
        for rest in rests:
            block = block + rest[a * T : (a + 1) * T, :].astype(f32)
        out[:T, :] = block.astype(out.dtype)
        if extra:
            out[T:, :] = three_parts(total) if out.dtype == bf16 else one_row(total)


def join_kernel(extra, mine, other, *outs):
    if extra:
        total = jnp.sum(mine[0, T:, :] + other[0, T:, :], axis=0, keepdims=True)
    for k, out in enumerate(outs):
        out[:T, :] = (mine[k, :T, :] + other[k, :T, :]).astype(out.dtype)
        if extra:
            out[T:, :] = three_parts(total) if k else one_row(total)


def block_sum(refs):
    total = refs[0][:T, :].astype(f32)
    for ref in refs[1:]:
        total = total + ref[:T, :].astype(f32)
    return total


def rest_kernel(extra, *refs):
    near, out = refs[:N4], refs[N4]
    for a in range(1, N4):
        out[(a - 1) * T : a * T, :] = near[a][:T, :]
    if extra:
        out[REST:, :] = three_parts(sum_of_parts(near))


BLOCKS = 2 * N4 - 1


def primal_one_kernel(*refs):
    grads, (x, cost, low, high, step, primal, ahead) = refs[:BLOCKS], refs[BLOCKS:]
    grad = block_sum(grads).T
    one = jnp.clip(x[...] - step[...] * (cost[...] - grad), low[...], high[...])
    primal[...] = one
    diff = one - x[...]
    ahead[:T, :] = (2.0 * one - x[...]).astype(bf16)
    ahead[T:, :] = three_parts(jnp.sum(diff * diff, axis=0, keepdims=True))


def dual_one_kernel(*refs):
    images, (y, side, step, dual, moved, flipped) = refs[:N4], refs[N4:]
    image = block_sum(images)
    moved[...] = sum_of_parts(images[:1]) + sum_of_parts(images[1:])
    one = jnp.maximum(y[...] + step[...] * (side[...] - image), 0.0)
    dual[...] = one
    diff = one - y[...]
    flipped[:T, :] = one.T.astype(bf16)
    flipped[T:, :] = three_parts(jnp.sum(diff * diff, axis=0, keepdims=True))


def primal_two_kernel(rows, cols, *refs):
    grads = refs[:BLOCKS]
    line, moved, one, cost, low, high, step, primal, weight, ahead = refs[BLOCKS:]
    grad = block_sum(grads).T
    move_dual = line[...] + sum_of_parts(grads[N4:])
    w = jnp.sqrt((move_dual / rows + EPS) / (moved[...] / cols + EPS))
    weight[...] = w
    two = jnp.clip(one[...] - step[...] / w * (cost[...] - grad), low[...], high[...])
    primal[...] = two
    ahead[...] = (2.0 * two - one[...]).astype(bf16)


def dual_two_kernel(*refs):
    images, (one, side, step, weight, dual) = refs[:N4], refs[N4:]
    dual[...] = jnp.maximum(one[...] + step[...] * weight[...] * (side[...] - block_sum(images)), 0.0)


def flip_kernel(y, flipped):
    flipped[...] = y[...].T.astype(bf16)


def permute(value, places):
    return lax.ppermute(value, ROW_COL, [(flat(p), flat(q)) for p, q in places])


def flat(place):
    y, z, x, core = place
    return ((y * N4 + z) * N4 + x) * 2 + core


EVERYONE = [(y, z, x, core) for y in range(N4) for z in range(N4) for x in range(N4) for core in range(2)]


def along_y(p, k):
    return ((p[0] + k) % N4, *p[1:])


def along_z(p, k):
    return (p[0], (p[1] + k) % N4, *p[2:])


def to_big(value, k):
    return permute(value, [(p, along_y(p, k) if p[3] else along_z(p, k)) for p in EVERYONE])


def to_small(value, k):
    return permute(value, [(p, along_z(p, k) if p[3] else along_y(p, k)) for p in EVERYONE])


def to_x(value, k):
    return permute(value, [(p, (*p[:2], (p[2] + k) % N4, p[3])) for p in EVERYONE])


def to_other_core(value):
    return permute(value, [(p, (*p[:3], 1 - p[3])) for p in EVERYONE])


FAR_FIRST = (1, 3, 2)


START_ORDER = (1, 3, 2)


def sent(values, send):
    arrived = {}
    for k in START_ORDER:
        arrived[k] = send(values[k - 1], k)
    return [arrived[k] for k in range(1, N4)]


def body(
    matrix_tiles,
    tile_rows,
    tile_cols,
    tile_count,
    x_start,
    y_start,
    cost_vector,
    right_side,
    lower_bound,
    upper_bound,
    step_primal,
    step_dual,
):
    dense = make_dense(tile_rows, tile_cols, tile_count, matrix_tiles)
    everyone = lax.axis_size(ROW) * lax.axis_size(COL)
    total_cols = x_start.shape[0] * everyone
    total_rows = y_start.shape[0] * everyone
    step_p, step_d = step_primal[None], step_dual[None]
    square = ((T, T), f32)
    line = ((1, T), f32)

    def to_columns(flipped, extra, ready=None):
        mine = [flipped] + sent([flipped] * 3, to_x)
        if ready is not None:
            mine[0], ready = lax.optimization_barrier((flipped, ready))
        matrix = dense if ready is None else ready
        pieces = mine + [to_other_core(piece) for piece in mine]
        rests = {k: backward_rest(matrix, pieces, k, extra) for k in FAR_FIRST}
        rests = sent([rests[k] for k in range(1, N4)], to_big)
        own, own_rest, moved, firsts = backward_near(matrix, pieces, extra)
        firsts = sent(firsts, to_big)
        block = ((WIDE, T), f32) if extra else ((T, T), bf16)
        *blocks, moved = call(lambda *refs: big_sum_kernel(extra, *refs), [block] * 3 + [line], own_rest, moved, *rests)
        return [own, *firsts, *sent(blocks, to_small)], moved

    def to_rows(ahead, extra):
        near = [ahead] + sent([ahead] * 3, to_small)
        firsts = sent([ahead] * 3, to_big)
        tall = TALL if extra else T
        (rest,) = call(lambda *refs: rest_kernel(extra, *refs), [((REST + tall - T, T), bf16)], *near)
        rests = sent([rest] * 3, to_big)
        early = forward_early(dense, near, firsts)
        other = to_other_core(forward_late(dense, early, near, rests, True, extra))
        mine = forward_late(dense, early, near, rests, False, extra)
        outs = [((WIDE if extra else T, T), f32)] + [((tall, T), bf16)] * (N4 - 1)
        own, *blocks = call(lambda *refs: join_kernel(extra, *refs), outs, mine, other)
        return [own, *sent(blocks, to_x)]

    (flipped,) = call(flip_kernel, [((T, T), bf16)], y_start)
    grads, _ = to_columns(flipped, False, dense)
    one, ahead = call(
        primal_one_kernel,
        [square, ((TALL, T), bf16)],
        *grads, x_start, cost_vector, lower_bound, upper_bound, step_p,
    )
    images = to_rows(ahead, True)
    dual, moved, flipped = call(
        dual_one_kernel,
        [square, line, ((TALL, T), bf16)],
        *images, y_start, right_side, step_d,
    )
    grads, moved_line = to_columns(flipped, True)
    two, weight, ahead = call(
        lambda *refs: primal_two_kernel(float(total_rows), float(total_cols), *refs),
        [square, line, ((T, T), bf16)],
        *grads, moved_line, moved, one, cost_vector, lower_bound, upper_bound, step_p,
    )
    images = to_rows(ahead, False)
    (dual_out,) = call(dual_two_kernel, [square], *images, dual, right_side, step_d, weight)
    return (two, dual_out)


def solution(mesh):
    torus = Mesh(mesh.devices.reshape(4, 4, 4, 2), ("row_0", "row_1", "col_0", "col_1"))
    in_specs = (
        P(ROW, COL, None, None, None),
        P(ROW, COL, None),
        P(ROW, COL, None),
        P(ROW, COL),
        P(COL_ROW, None),
        P(ROW_COL, None),
        P(COL_ROW, None),
        P(ROW_COL, None),
        P(COL_ROW, None),
        P(COL_ROW, None),
        P(),
        P(),
    )
    out_specs = (P(COL_ROW, None), P(ROW_COL, None))
    return jax.shard_map(body, mesh=torus, in_specs=in_specs, out_specs=out_specs, check_vma=False)
```
